8 devices in a mesh: cp: 2 (over z, y), fsdp: 4 (over x, core).
Axes of the slice: x: 2, y: 2, z: 1, core: 2. Of those that a mesh axis runs over, the one named last changes fastest.
Arguments:
- act_in: bfloat16 [128, 128, 2048], P('fsdp', 'cp')
- grad_out: bfloat16 [128, 128, 2048], P('fsdp', 'cp')
- positions: int32 [128], P('cp')
- attn_norm: bfloat16 [2048], P(('fsdp', 'cp'))
- w_q: bfloat16 [2048, 32, 64], P(('fsdp', 'cp'))
- w_k: bfloat16 [2048, 4, 64], P(('fsdp', 'cp'))
- w_v: bfloat16 [2048, 4, 64], P(('fsdp', 'cp'))
- w_o: bfloat16 [2048, 2048], P(('fsdp', 'cp'))
- ffn_norm: bfloat16 [2048], P(('fsdp', 'cp'))
- w_gate: bfloat16 [2048, 5632], P(('fsdp', 'cp'))
- w_up: bfloat16 [2048, 5632], P(('fsdp', 'cp'))
- w_down: bfloat16 [5632, 2048], P(('fsdp', 'cp'))
Outputs:
- output 1: bfloat16 [128, 128, 2048], P('fsdp', 'cp')
- output 2: bfloat16 [128, 128, 2048], P('fsdp', 'cp')
- output 3: float32 [2048], P(('fsdp', 'cp'))
- output 4: float32 [2048, 32, 64], P(('fsdp', 'cp'))
- output 5: float32 [2048, 4, 64], P(('fsdp', 'cp'))
- output 6: float32 [2048, 4, 64], P(('fsdp', 'cp'))
- output 7: float32 [2048, 2048], P(('fsdp', 'cp'))
- output 8: float32 [2048], P(('fsdp', 'cp'))
- output 9: float32 [2048, 5632], P(('fsdp', 'cp'))
- output 10: float32 [2048, 5632], P(('fsdp', 'cp'))
- output 11: float32 [5632, 2048], P(('fsdp', 'cp'))
All inputs are finite; a program needn't handle non-finite values.
Results may differ from the reference program's by a relative error of at most 0.0147092.
Values are sent between devices in bfloat16 or wider.
A program may use at most 1 GiB of HBM per device.

```python
import functools
import jax
import jax.numpy as jnp
from jax import lax

BATCH_SIZE = 128
SEQ_LEN = 128
MODEL_DIM = 2048
NUM_HEADS = 32
KV_HEADS = 4
HEAD_DIM = 64
FFN_DIM = 5632
NUM_DEVICES = 8
NORM_EPS = 1e-5
ROPE_THETA = 500000.0
NEG_INF = -1e30


def normal_weight(key, shape, fan_in):
    return (jax.random.normal(key, shape, jnp.float32) * fan_in ** -0.5).astype(jnp.bfloat16)


def setup_inputs(seed: int = 0) -> dict:
    keys = jax.random.split(jax.random.key(seed), 12)
    act_shape = (BATCH_SIZE, SEQ_LEN, MODEL_DIM)
    return {
        "act_in": jax.random.normal(keys[0], act_shape, jnp.float32).astype(jnp.bfloat16),
        "grad_out": jax.random.normal(keys[1], act_shape, jnp.float32).astype(jnp.bfloat16),
        "positions": jax.random.permutation(keys[2], SEQ_LEN).astype(jnp.int32),
        "attn_norm": (1.0 + 0.3 * jax.random.normal(keys[3], (MODEL_DIM,), jnp.float32)).astype(jnp.bfloat16),
        "w_q": normal_weight(keys[4], (MODEL_DIM, NUM_HEADS, HEAD_DIM), MODEL_DIM),
        "w_k": normal_weight(keys[5], (MODEL_DIM, KV_HEADS, HEAD_DIM), MODEL_DIM),
        "w_v": normal_weight(keys[6], (MODEL_DIM, KV_HEADS, HEAD_DIM), MODEL_DIM),
        "w_o": normal_weight(keys[7], (NUM_HEADS * HEAD_DIM, MODEL_DIM), NUM_HEADS * HEAD_DIM),
        "ffn_norm": (1.0 + 0.3 * jax.random.normal(keys[8], (MODEL_DIM,), jnp.float32)).astype(jnp.bfloat16),
        "w_gate": normal_weight(keys[9], (MODEL_DIM, FFN_DIM), MODEL_DIM),
        "w_up": normal_weight(keys[10], (MODEL_DIM, FFN_DIM), MODEL_DIM),
        "w_down": normal_weight(keys[11], (FFN_DIM, MODEL_DIM), FFN_DIM),
    }


def rms_norm(hidden, gain):
    hid32 = hidden.astype(jnp.float32)
    inv_rms = lax.rsqrt(jnp.mean(hid32 * hid32, axis=-1, keepdims=True) + NORM_EPS)
    return (hid32 * inv_rms * gain.astype(jnp.float32)).astype(jnp.bfloat16)


def rope_tables(positions):
    half = HEAD_DIM // 2
    inv_freq = jnp.power(ROPE_THETA, -(jnp.arange(half, dtype=jnp.float32) * (2.0 / HEAD_DIM)))
    angle = positions.astype(jnp.float32)[:, None] * inv_freq[None, :]
    return jnp.cos(angle), jnp.sin(angle)


def rotate(vals, cos_t, sin_t):
    half = vals.shape[-1] // 2
    table_shape = (cos_t.shape[0],) + (1,) * (vals.ndim - 3) + (half,)
    cos_b = cos_t.reshape(table_shape)
    sin_b = sin_t.reshape(table_shape)
    first = vals[..., :half]
    second = vals[..., half:]
    return jnp.concatenate([first * cos_b - second * sin_b, second * cos_b + first * sin_b], axis=-1)


def project(act, weight):
    lead = act.shape[:-1]
    flat = jnp.dot(act.reshape(-1, act.shape[-1]), weight.astype(jnp.bfloat16).reshape(weight.shape[0], -1), preferred_element_type=jnp.float32)
    return flat.reshape(lead + weight.shape[1:])


def layer(positions, act_in, attn_norm, w_q, w_k, w_v, w_o, ffn_norm, w_gate, w_up, w_down):
    batch, seq_len = act_in.shape[0], act_in.shape[1]
    groups = NUM_HEADS // KV_HEADS
    cos_t, sin_t = rope_tables(positions)
    normed = rms_norm(act_in, attn_norm)
    query = project(normed, w_q).reshape(batch, seq_len, KV_HEADS, groups, HEAD_DIM)
    query = rotate(query, cos_t, sin_t).astype(jnp.bfloat16)
    key_rot = rotate(project(normed, w_k), cos_t, sin_t).astype(jnp.bfloat16)
    value = project(normed, w_v).astype(jnp.bfloat16)
    scores = jnp.einsum("bqkgd,bskd->bkgqs", query.astype(jnp.float32), key_rot.astype(jnp.float32)) * HEAD_DIM ** -0.5
    scores = jnp.where(positions[None, :] <= positions[:, None], scores, NEG_INF)
    attn_prob = jax.nn.softmax(scores, axis=-1).astype(jnp.bfloat16)
    attn_ctx = jnp.einsum("bkgqs,bskd->bqkgd", attn_prob.astype(jnp.float32), value.astype(jnp.float32)).astype(jnp.bfloat16)
    attn_proj = project(attn_ctx.reshape(batch, seq_len, NUM_HEADS * HEAD_DIM), w_o)
    resid = (act_in.astype(jnp.float32) + attn_proj).astype(jnp.bfloat16)
    normed2 = rms_norm(resid, ffn_norm)
    hidden = (jax.nn.silu(project(normed2, w_gate)) * project(normed2, w_up)).astype(jnp.bfloat16)
    return (resid.astype(jnp.float32) + project(hidden, w_down)).astype(jnp.bfloat16)


def reference(act_in, grad_out, positions, attn_norm, w_q, w_k, w_v, w_o, ffn_norm, w_gate, w_up, w_down):
    params = [weight.astype(jnp.float32) for weight in (attn_norm, w_q, w_k, w_v, w_o, ffn_norm, w_gate, w_up, w_down)]
    act_out, pull = jax.vjp(functools.partial(layer, positions), act_in, *params)
    grads = pull(grad_out)
    return (act_out, grads[0], grads[1] / NUM_DEVICES, grads[2] / NUM_DEVICES, grads[3] / NUM_DEVICES, grads[4] / NUM_DEVICES, grads[5] / NUM_DEVICES, grads[6] / NUM_DEVICES, grads[7] / NUM_DEVICES, grads[8] / NUM_DEVICES, grads[9] / NUM_DEVICES)
```

```python
import functools

import jax
import jax.numpy as jnp
from jax import lax
from jax.experimental import pallas as pl
from jax.experimental.pallas import tpu as pltpu
from jax.sharding import PartitionSpec as P


NORM_EPS = 1e-5
ROPE_THETA = 500000.0
NEG_INF = -1e30
SHARD_AXES = ("fsdp", "cp")
LANES = 128
HALF_SLAB = 64


def matmul(form, lhs, rhs):
    return jnp.einsum(form, lhs, rhs, preferred_element_type=jnp.float32)


def dims(lhs_dim, rhs_dim):
    return (((lhs_dim,), (rhs_dim,)), ((), ()))


def kdot(lhs, rhs, lhs_dim, rhs_dim):
    return lax.dot_general(lhs, rhs, dims(lhs_dim, rhs_dim), preferred_element_type=jnp.float32)


def lane_of(rows):
    return lax.broadcasted_iota(jnp.int32, (rows, LANES), 1)


def partner_half(vals):
    low = (lane_of(vals.shape[0]) % 64) < 32
    return jnp.where(low, pltpu.roll(vals, LANES - 32, 1), pltpu.roll(vals, 32, 1))


def pair_blocks(slab, odd):
    wide = slab.astype(jnp.float32)
    low = lane_of(wide.shape[0]) < HALF_SLAB
    mine = jnp.where(low, 0.0, wide) if odd else jnp.where(low, wide, 0.0)
    moved = pltpu.roll(mine, HALF_SLAB, 1)
    parts = (moved, mine) if odd else (mine, moved)
    return jnp.concatenate(parts, axis=0).astype(jnp.bfloat16)


def rope_kv_kernel(kv_ref, cos_ref, sin_ref, out_ref):
    reps = kv_ref.shape[0] // cos_ref.shape[0]
    cos_t = jnp.concatenate([cos_ref[...]] * reps, axis=0)
    sin_t = jnp.concatenate([sin_ref[...]] * reps, axis=0)
    for j in range(2):
        cols = slice(j * LANES, (j + 1) * LANES)
        vals = kv_ref[:, cols]
        out_ref[:, cols] = (vals * cos_t + partner_half(vals) * sin_t).astype(jnp.bfloat16)
    out_ref[:, 2 * LANES:] = kv_ref[:, 2 * LANES:].astype(jnp.bfloat16)


def unrope_kv_kernel(own_ref, got_ref, cos_ref, sin_ref, wide_ref, out_ref):
    del wide_ref
    reps = own_ref.shape[0] // cos_ref.shape[0]
    cos_t = jnp.concatenate([cos_ref[...]] * reps, axis=0)
    sin_t = jnp.concatenate([sin_ref[...]] * reps, axis=0)
    for j in range(2):
        cols = slice(j * LANES, (j + 1) * LANES)
        vals = own_ref[:, cols] + got_ref[:, cols]
        out_ref[:, cols] = (vals * cos_t - partner_half(vals) * sin_t).astype(jnp.bfloat16)
    out_ref[:, 2 * LANES:] = (own_ref[:, 2 * LANES:] + got_ref[:, 2 * LANES:]).astype(jnp.bfloat16)


def stack_slabs(ref, group):
    return jnp.concatenate([ref[:, pl.ds((group * 4 + j) * LANES, LANES)] for j in range(4)], axis=0)


def write_slabs(ref, group, vals):
    rows = vals.shape[0] // 4
    for j in range(4):
        ref[:, pl.ds((group * 4 + j) * LANES, LANES)] = vals[j * rows:(j + 1) * rows].astype(ref.dtype)


def kv_pair(kv_ref, kvo_ref, group):
    at = (group // 2) * LANES
    odd = group % 2 == 1
    key = jnp.concatenate([kv_ref[:, at:at + LANES], kvo_ref[:, at:at + LANES]], axis=0)
    at += 2 * LANES
    val = jnp.concatenate([kv_ref[:, at:at + LANES], kvo_ref[:, at:at + LANES]], axis=0)
    return pair_blocks(key, odd), pair_blocks(val, odd)


def softmax_pair(query, key2, mask, scale):
    scores = kdot(query, key2, 1, 1) * scale
    probs = []
    for j in range(2):
        part = jnp.where(mask, scores[:, j * LANES:(j + 1) * LANES], NEG_INF)
        expo = jnp.exp(part - jnp.max(part, axis=1, keepdims=True))
        probs.append(expo * (1.0 / jnp.sum(expo, axis=1, keepdims=True)))
    return probs


def attn_fwd_kernel(scale, q_ref, kv_ref, kvo_ref, cos_ref, sin_ref, mask_ref, ctx_ref, qb_ref):
    mask = mask_ref[...] > 0.0
    for group in range(4):
        key2, val2 = kv_pair(kv_ref, kvo_ref, group)
        raw = stack_slabs(q_ref, group)
        query = (raw * cos_ref[...] + partner_half(raw) * sin_ref[...]).astype(jnp.bfloat16)
        write_slabs(qb_ref, group, query)
        probs = softmax_pair(query, key2, mask, scale)
        prob = jnp.concatenate([part.astype(jnp.bfloat16) for part in probs], axis=1)
        write_slabs(ctx_ref, group, kdot(prob, val2, 1, 0))


def attn_bwd_kernel(scale, qb_ref, dc_ref, kv_ref, kvo_ref, cos_ref, sin_ref, mask_ref, dq_ref, own_ref, oth_ref):
    mask = mask_ref[...] > 0.0
    keys = 2 * kv_ref.shape[0]
    local = kv_ref.shape[0]
    low = lane_of(keys) < HALF_SLAB
    held = {}
    for group in range(4):
        key2, val2 = kv_pair(kv_ref, kvo_ref, group)
        query = stack_slabs(qb_ref, group)
        d_ctx = stack_slabs(dc_ref, group)
        probs = softmax_pair(query, key2, mask, scale)
        d_prob = kdot(d_ctx, val2, 1, 1)
        d_scores = []
        for j in range(2):
            part = d_prob[:, j * LANES:(j + 1) * LANES]
            inner = jnp.sum(probs[j] * part, axis=1, keepdims=True)
            d_scores.append((probs[j] * (part - inner) * scale).astype(jnp.bfloat16))
        d_score = jnp.concatenate(d_scores, axis=1)
        prob = jnp.concatenate([part.astype(jnp.bfloat16) for part in probs], axis=1)
        d_query = kdot(d_score, key2, 1, 0)
        write_slabs(dq_ref, group, d_query * cos_ref[...] - partner_half(d_query) * sin_ref[...])
        for which, (lhs, rhs) in enumerate(((d_score, query), (prob, d_ctx))):
            both = kdot(lhs, rhs, 0, 0)
            top, bottom = both[:keys], both[keys:]
            if group % 2 == 0:
                held[which] = top + pltpu.roll(bottom, HALF_SLAB, 1)
            else:
                slab = jnp.where(low, held[which], bottom + pltpu.roll(top, HALF_SLAB, 1))
                at = (2 * which + group // 2) * LANES
                own_ref[:, at:at + LANES] = slab[:local]
                oth_ref[:, at:at + LANES] = slab[local:]


def cost(flops, nbytes):
    return pl.CostEstimate(flops=int(flops), bytes_accessed=int(nbytes), transcendentals=0)


VMEM_LIMIT = 48 * 1024 * 1024


def params():
    return pltpu.CompilerParams(dimension_semantics=("arbitrary",), vmem_limit_bytes=VMEM_LIMIT)


def norm_fwd(hidden, gain):
    hid32 = hidden.astype(jnp.float32)
    inv_rms = lax.rsqrt(jnp.mean(hid32 * hid32, axis=-1, keepdims=True) + NORM_EPS)
    return (hid32 * inv_rms * gain).astype(jnp.bfloat16), inv_rms


def norm_bwd(d_normed, hidden, inv_rms, gain):
    unit = hidden.astype(jnp.float32) * inv_rms
    d_unit = d_normed * gain
    d_hidden = inv_rms * (d_unit - unit * jnp.mean(d_unit * unit, axis=-1, keepdims=True))
    return d_hidden, jnp.sum(d_normed * unit, axis=0)


def gather_weight(shard):
    return lax.all_gather(shard, SHARD_AXES, axis=0, tiled=True)


def scatter_grad(local_grad):
    return lax.psum_scatter(local_grad, SHARD_AXES, scatter_dimension=0, tiled=True)


def solution(mesh):
    n_dev = mesh.shape["fsdp"] * mesh.shape["cp"]
    act_spec = P("fsdp", "cp", None)
    vec_spec = P(SHARD_AXES)
    mat_spec = P(SHARD_AXES, None)
    cube_spec = P(SHARD_AXES, None, None)
    bf16, f32 = jnp.bfloat16, jnp.float32

    def body(act_in, grad_out, positions, attn_norm, w_q, w_k, w_v, w_o, ffn_norm, w_gate, w_up, w_down):
        batch, seq, width = act_in.shape
        heads, head_dim = w_q.shape[1], w_q.shape[2]
        kv_heads = w_k.shape[1]
        rows = w_q.shape[0]
        q_cols, kv_cols = heads * head_dim, kv_heads * head_dim
        tokens = batch * seq
        scale = head_dim ** -0.5
        x = act_in.reshape(tokens, width)
        dy = grad_out.reshape(tokens, width)

        pos_f = jnp.concatenate([positions.astype(f32), jnp.zeros((rows - seq,), f32)])
        small = jnp.stack([attn_norm.astype(f32), ffn_norm.astype(f32), pos_f])
        small = lax.all_gather(small, SHARD_AXES, axis=0)
        gain1 = small[:, 0].reshape(-1)
        gain2 = small[:, 1].reshape(-1)
        pos_own = positions.astype(f32)
        pos_oth = jnp.where(lax.axis_index("cp") == 0, small[1, 2, :seq], small[0, 2, :seq])

        full_qkv = gather_weight(jnp.concatenate(
            [w_q.reshape(rows, q_cols), w_k.reshape(rows, kv_cols), w_v.reshape(rows, kv_cols)], axis=1))
        full_o = gather_weight(w_o)
        full_gate = gather_weight(w_gate)
        full_up = gather_weight(w_up)
        full_down = gather_weight(w_down)

        half = head_dim // 2
        inv_freq = jnp.power(ROPE_THETA, -(jnp.arange(half, dtype=f32) * (2.0 / head_dim)))
        angle = pos_own[:, None] * inv_freq[None, :]
        cos_t, sin_t = jnp.cos(angle), jnp.sin(angle)
        cos_t = jnp.concatenate([cos_t] * 4, axis=1)
        sin_t = jnp.concatenate([-sin_t, sin_t, -sin_t, sin_t], axis=1)
        cos_4, sin_4 = jnp.concatenate([cos_t] * 4, axis=0), jnp.concatenate([sin_t] * 4, axis=0)
        pos_keys = jnp.concatenate([pos_own, pos_oth])
        mask = (pos_keys[None, :] <= pos_own[:, None]).astype(f32)
        mask_4 = jnp.concatenate([mask] * 4, axis=0)

        whole = lambda arr: pl.BlockSpec(arr.shape, lambda b: (0, 0))
        q_blk = pl.BlockSpec((seq, q_cols), lambda b: (b, 0))
        kv_blk = pl.BlockSpec((seq, 2 * kv_cols), lambda b: (b, 0))
        t_blk = 4 * seq
        kv_in_blk = pl.BlockSpec((t_blk, 2 * kv_cols), lambda b: (b, q_cols // (2 * kv_cols)))
        kv_tall = pl.BlockSpec((t_blk, 2 * kv_cols), lambda b: (b, 0))
        pair_flops = 2 * tokens * heads * head_dim * 2 * seq

        normed, rms1 = norm_fwd(x, gain1)
        qkv = matmul("td,dn->tn", normed, full_qkv)
        kv = pl.pallas_call(
            rope_kv_kernel, grid=(tokens // t_blk,),
            in_specs=[kv_in_blk, whole(cos_t), whole(sin_t)], out_specs=kv_tall,
            out_shape=jax.ShapeDtypeStruct((tokens, 2 * kv_cols), bf16),
            compiler_params=params(), cost_estimate=cost(1e9, 6e6), name="rope_kv",
        )(qkv, cos_t, sin_t)
        swap = [(0, 1), (1, 0)]
        kv_oth = lax.ppermute(kv, "cp", swap)
        ctx, query = pl.pallas_call(
            functools.partial(attn_fwd_kernel, scale), grid=(batch,),
            in_specs=[q_blk, kv_blk, kv_blk, whole(cos_4), whole(sin_4), whole(mask_4)],
            out_specs=[q_blk, q_blk],
            out_shape=[jax.ShapeDtypeStruct((tokens, q_cols), bf16)] * 2,
            compiler_params=params(), cost_estimate=cost(4 * pair_flops, 40e6), name="attn_fwd",
        )(qkv, kv, kv_oth, cos_4, sin_4, mask_4)
        resid = (x.astype(f32) + matmul("tn,nd->td", ctx, full_o)).astype(bf16)
        normed2, rms2 = norm_fwd(resid, gain2)
        gate_pre = matmul("td,df->tf", normed2, full_gate)
        up_pre = matmul("td,df->tf", normed2, full_up)
        gate_sig = jax.nn.sigmoid(gate_pre)
        gate_act = gate_pre * gate_sig
        hidden = (gate_act * up_pre).astype(bf16)

        grad_down = matmul("tf,td->fd", hidden, dy)
        grad_down, dy, hidden = lax.optimization_barrier((grad_down, dy, hidden))
        grad_down = scatter_grad(grad_down) / n_dev
        d_hidden = matmul("td,fd->tf", dy, full_down)
        d_gate = (d_hidden * up_pre * gate_sig * (1.0 + gate_pre * (1.0 - gate_sig))).astype(bf16)
        d_up = (d_hidden * gate_act).astype(bf16)
        grad_gate = matmul("td,tf->df", normed2, d_gate)
        grad_gate, d_up = lax.optimization_barrier((grad_gate, d_up))
        grad_gate = scatter_grad(grad_gate) / n_dev
        grad_up = matmul("td,tf->df", normed2, d_up)
        grad_up, d_gate, d_up, hidden = lax.optimization_barrier((grad_up, d_gate, d_up, hidden))
        grad_up = scatter_grad(grad_up) / n_dev
        d_normed2 = matmul("tf,df->td", d_gate, full_gate)
        d_normed2 = d_normed2 + matmul("tf,df->td", d_up, full_up)
        d_resid, grad_ffn = norm_bwd(d_normed2, resid, rms2, gain2)
        d_resid = d_resid + dy.astype(f32)
        d_resid_half = d_resid.astype(bf16)
        grad_o = matmul("tn,td->nd", ctx, d_resid_half)
        grad_o, d_resid_half = lax.optimization_barrier((grad_o, d_resid_half))
        grad_o = scatter_grad(grad_o) / n_dev
        d_ctx = matmul("td,nd->tn", d_resid_half, full_o).astype(bf16)
        dq_wide, dkv_own, dkv_oth = pl.pallas_call(
            functools.partial(attn_bwd_kernel, scale), grid=(batch,),
            in_specs=[q_blk, q_blk, kv_blk, kv_blk, whole(cos_4), whole(sin_4), whole(mask_4)],
            out_specs=[q_blk, kv_blk, kv_blk],
            out_shape=[jax.ShapeDtypeStruct((tokens, q_cols + 2 * kv_cols), bf16)]
            + [jax.ShapeDtypeStruct((tokens, 2 * kv_cols), f32)] * 2,
            compiler_params=params(), cost_estimate=cost(10 * pair_flops, 50e6), name="attn_bwd",
        )(query, d_ctx, kv, kv_oth, cos_4, sin_4, mask_4)
        dkv_got = lax.ppermute(dkv_oth, "cp", swap)
        act_out = (resid.astype(f32) + matmul("tf,fd->td", hidden, full_down)).astype(bf16)
        d_qkv = pl.pallas_call(
            unrope_kv_kernel, grid=(tokens // t_blk,),
            in_specs=[kv_tall, kv_tall, whole(cos_t), whole(sin_t), pl.BlockSpec(memory_space=pl.ANY)],
            out_specs=kv_in_blk,
            out_shape=jax.ShapeDtypeStruct(dq_wide.shape, bf16),
            input_output_aliases={4: 0},
            compiler_params=params(), cost_estimate=cost(1e9, 10e6), name="unrope_kv",
        )(dkv_own, dkv_got, cos_t, sin_t, dq_wide)
        grad_qkv = matmul("td,tn->dn", normed, d_qkv)
        grad_qkv, d_qkv = lax.optimization_barrier((grad_qkv, d_qkv))
        grad_qkv = scatter_grad(grad_qkv) / n_dev
        d_normed = matmul("tn,dn->td", d_qkv, full_qkv)
        d_input, grad_attn = norm_bwd(d_normed, x, rms1, gain1)
        grad_in = (d_resid + d_input).astype(bf16)
        gains = jnp.stack([grad_attn.reshape(n_dev, rows), grad_ffn.reshape(n_dev, rows)], axis=1)
        gains = lax.psum_scatter(gains, SHARD_AXES, scatter_dimension=0, tiled=True)[0] / n_dev
        grad_q = grad_qkv[:, :q_cols].reshape(w_q.shape)
        grad_k = grad_qkv[:, q_cols:q_cols + kv_cols].reshape(w_k.shape)
        grad_v = grad_qkv[:, q_cols + kv_cols:].reshape(w_v.shape)
        shape = act_in.shape
        return (act_out.reshape(shape), grad_in.reshape(shape), gains[0], grad_q, grad_k, grad_v, grad_o, gains[1],
                grad_gate, grad_up, grad_down)

    in_specs = (act_spec, act_spec, P("cp"), vec_spec, cube_spec, cube_spec, cube_spec, mat_spec, vec_spec, mat_spec, mat_spec, mat_spec)
    out_specs = (act_spec, act_spec, vec_spec, cube_spec, cube_spec, cube_spec, mat_spec, vec_spec, mat_spec, mat_spec, mat_spec)
    return jax.shard_map(body, mesh=mesh, in_specs=in_specs, out_specs=out_specs, check_vma=False)
```

```python
import functools

import jax
import jax.numpy as jnp
from jax import lax
from jax.experimental import pallas as pl
from jax.experimental.pallas import tpu as pltpu
from jax.sharding import PartitionSpec as P


NORM_EPS = 1e-5
ROPE_THETA = 500000.0
NEG_INF = -1e30
SHARD_AXES = ("fsdp", "cp")
LANES = 128
HALF_SLAB = 64


def matmul(form, lhs, rhs):
    return jnp.einsum(form, lhs, rhs, preferred_element_type=jnp.float32)


def dims(lhs_dim, rhs_dim):
    return (((lhs_dim,), (rhs_dim,)), ((), ()))


def kdot(lhs, rhs, lhs_dim, rhs_dim):
    return lax.dot_general(lhs, rhs, dims(lhs_dim, rhs_dim), preferred_element_type=jnp.float32)


def lane_of(rows):
    return lax.broadcasted_iota(jnp.int32, (rows, LANES), 1)


def partner_half(vals):
    low = (lane_of(vals.shape[0]) % 64) < 32
    return jnp.where(low, pltpu.roll(vals, LANES - 32, 1), pltpu.roll(vals, 32, 1))


def pair_blocks(slab, odd):
    wide = slab.astype(jnp.float32)
    low = lane_of(wide.shape[0]) < HALF_SLAB
    mine = jnp.where(low, 0.0, wide) if odd else jnp.where(low, wide, 0.0)
    moved = pltpu.roll(mine, HALF_SLAB, 1)
    parts = (moved, mine) if odd else (mine, moved)
    return jnp.concatenate(parts, axis=0).astype(jnp.bfloat16)


def rope_kv_kernel(kv_ref, cos_ref, sin_ref, out_ref):
    reps = kv_ref.shape[0] // cos_ref.shape[0]
    cos_t = jnp.concatenate([cos_ref[...]] * reps, axis=0)
    sin_t = jnp.concatenate([sin_ref[...]] * reps, axis=0)
    for j in range(2):
        cols = slice(j * LANES, (j + 1) * LANES)
        vals = kv_ref[:, cols]
        out_ref[:, cols] = (vals * cos_t + partner_half(vals) * sin_t).astype(jnp.bfloat16)
    out_ref[:, 2 * LANES:] = kv_ref[:, 2 * LANES:].astype(jnp.bfloat16)


def unrope_kv_kernel(own_ref, got_ref, cos_ref, sin_ref, wide_ref, out_ref):
    del wide_ref
    reps = own_ref.shape[0] // cos_ref.shape[0]
    cos_t = jnp.concatenate([cos_ref[...]] * reps, axis=0)
    sin_t = jnp.concatenate([sin_ref[...]] * reps, axis=0)
    for j in range(2):
        cols = slice(j * LANES, (j + 1) * LANES)
        vals = own_ref[:, cols] + got_ref[:, cols]
        out_ref[:, cols] = (vals * cos_t - partner_half(vals) * sin_t).astype(jnp.bfloat16)
    out_ref[:, 2 * LANES:] = (own_ref[:, 2 * LANES:] + got_ref[:, 2 * LANES:]).astype(jnp.bfloat16)


def stack_slabs(ref, group):
    return jnp.concatenate([ref[:, pl.ds((group * 4 + j) * LANES, LANES)] for j in range(4)], axis=0)


def write_slabs(ref, group, vals):
    rows = vals.shape[0] // 4
    for j in range(4):
        ref[:, pl.ds((group * 4 + j) * LANES, LANES)] = vals[j * rows:(j + 1) * rows].astype(ref.dtype)


def kv_pair(kv_ref, kvo_ref, group):
    at = (group // 2) * LANES
    odd = group % 2 == 1
    key = jnp.concatenate([kv_ref[:, at:at + LANES], kvo_ref[:, at:at + LANES]], axis=0)
    at += 2 * LANES
    val = jnp.concatenate([kv_ref[:, at:at + LANES], kvo_ref[:, at:at + LANES]], axis=0)
    return pair_blocks(key, odd), pair_blocks(val, odd)


def softmax_pair(query, key2, mask, scale):
    scores = kdot(query, key2, 1, 1) * scale
    probs = []
    for j in range(2):
        part = jnp.where(mask, scores[:, j * LANES:(j + 1) * LANES], NEG_INF)
        expo = jnp.exp(part - jnp.max(part, axis=1, keepdims=True))
        probs.append(expo * (1.0 / jnp.sum(expo, axis=1, keepdims=True)))
    return probs


def attn_fwd_kernel(scale, q_ref, kv_ref, kvo_ref, cos_ref, sin_ref, mask_ref, ctx_ref, qb_ref):
    mask = mask_ref[...] > 0.0
    for group in range(4):
        key2, val2 = kv_pair(kv_ref, kvo_ref, group)
        raw = stack_slabs(q_ref, group)
        query = (raw * cos_ref[...] + partner_half(raw) * sin_ref[...]).astype(jnp.bfloat16)
        write_slabs(qb_ref, group, query)
        probs = softmax_pair(query, key2, mask, scale)
        prob = jnp.concatenate([part.astype(jnp.bfloat16) for part in probs], axis=1)
        write_slabs(ctx_ref, group, kdot(prob, val2, 1, 0))


def attn_bwd_kernel(scale, qb_ref, dc_ref, kv_ref, kvo_ref, cos_ref, sin_ref, mask_ref, dq_ref, own_ref, oth_ref):
    mask = mask_ref[...] > 0.0
    keys = 2 * kv_ref.shape[0]
    local = kv_ref.shape[0]
    low = lane_of(keys) < HALF_SLAB
    held = {}
    for group in range(4):
        key2, val2 = kv_pair(kv_ref, kvo_ref, group)
        query = stack_slabs(qb_ref, group)
        d_ctx = stack_slabs(dc_ref, group)
        probs = softmax_pair(query, key2, mask, scale)
        d_prob = kdot(d_ctx, val2, 1, 1)
        d_scores = []
        for j in range(2):
            part = d_prob[:, j * LANES:(j + 1) * LANES]
            inner = jnp.sum(probs[j] * part, axis=1, keepdims=True)
            d_scores.append((probs[j] * (part - inner) * scale).astype(jnp.bfloat16))
        d_score = jnp.concatenate(d_scores, axis=1)
        prob = jnp.concatenate([part.astype(jnp.bfloat16) for part in probs], axis=1)
        d_query = kdot(d_score, key2, 1, 0)
        write_slabs(dq_ref, group, d_query * cos_ref[...] - partner_half(d_query) * sin_ref[...])
        for which, (lhs, rhs) in enumerate(((d_score, query), (prob, d_ctx))):
            both = kdot(lhs, rhs, 0, 0)
            top, bottom = both[:keys], both[keys:]
            if group % 2 == 0:
                held[which] = top + pltpu.roll(bottom, HALF_SLAB, 1)
            else:
                slab = jnp.where(low, held[which], bottom + pltpu.roll(top, HALF_SLAB, 1))
                at = (2 * which + group // 2) * LANES
                own_ref[:, at:at + LANES] = slab[:local]
                oth_ref[:, at:at + LANES] = slab[local:]


def cost(flops, nbytes):
    return pl.CostEstimate(flops=int(flops), bytes_accessed=int(nbytes), transcendentals=0)


VMEM_LIMIT = 48 * 1024 * 1024


def params():
    return pltpu.CompilerParams(dimension_semantics=("arbitrary",), vmem_limit_bytes=VMEM_LIMIT)


def norm_fwd(hidden, gain):
    hid32 = hidden.astype(jnp.float32)
    inv_rms = lax.rsqrt(jnp.mean(hid32 * hid32, axis=-1, keepdims=True) + NORM_EPS)
    return (hid32 * inv_rms * gain).astype(jnp.bfloat16), inv_rms


def norm_bwd(d_normed, hidden, inv_rms, gain):
    unit = hidden.astype(jnp.float32) * inv_rms
    d_unit = d_normed * gain
    d_hidden = inv_rms * (d_unit - unit * jnp.mean(d_unit * unit, axis=-1, keepdims=True))
    return d_hidden, jnp.sum(d_normed * unit, axis=0)


def gather_weight(shard):
    return lax.all_gather(shard, SHARD_AXES, axis=0, tiled=True)


def scatter_grad(local_grad):
    return lax.psum_scatter(local_grad, SHARD_AXES, scatter_dimension=0, tiled=True)


SWAP_CORE = ("fsdp", [(0, 1), (1, 0), (2, 3), (3, 2)])
SWAP_X = ("fsdp", [(0, 2), (2, 0), (1, 3), (3, 1)])
SWAP_Y = ("cp", [(0, 1), (1, 0)])


def swap(vals, how):
    return lax.ppermute(vals, how[0], how[1])


def relative_blocks(lhs, order):
    block = lhs.shape[1] // 8
    place = lax.axis_index("fsdp")
    x_at, core, y_at = place // 2, place % 2, lax.axis_index("cp")
    sides = []
    for d_core in (0, 1):
        halves = []
        for first in (0, 1):
            for second in (0, 1):
                d_x, d_y = (first, second) if order == "x" else (second, first)
                owner = (((x_at + d_x) % 2) * 2 + (core + d_core) % 2) * 2 + (y_at + d_y) % 2
                halves.append(lax.dynamic_slice_in_dim(lhs, owner * block, block, 1))
        sides.append(halves)
    return sides


def partner_part(blocks, rhs, scale):
    return matmul("td,tn->dn", jnp.concatenate(blocks[1], axis=1), rhs) * scale


def own_parts(blocks, rhs, got, scale):
    cut = got.shape[0] // 2
    far = matmul("td,tn->dn", jnp.concatenate(blocks[0][2:], axis=1), rhs) * scale + got[cut:]
    near = matmul("td,tn->dn", jnp.concatenate(blocks[0][:2], axis=1), rhs) * scale + got[:cut]
    return far, near


def solution(mesh):
    n_dev = mesh.shape["fsdp"] * mesh.shape["cp"]
    act_spec = P("fsdp", "cp", None)
    vec_spec = P(SHARD_AXES)
    mat_spec = P(SHARD_AXES, None)
    cube_spec = P(SHARD_AXES, None, None)
    bf16, f32 = jnp.bfloat16, jnp.float32

    def body(act_in, grad_out, positions, attn_norm, w_q, w_k, w_v, w_o, ffn_norm, w_gate, w_up, w_down):
        batch, seq, width = act_in.shape
        heads, head_dim = w_q.shape[1], w_q.shape[2]
        kv_heads = w_k.shape[1]
        rows = w_q.shape[0]
        q_cols, kv_cols = heads * head_dim, kv_heads * head_dim
        tokens = batch * seq
        scale = head_dim ** -0.5
        share = 1.0 / n_dev
        x = act_in.reshape(tokens, width)
        dy = grad_out.reshape(tokens, width)

        pos_f = jnp.concatenate([positions.astype(f32), jnp.zeros((rows - seq,), f32)])
        small = jnp.stack([attn_norm.astype(f32), ffn_norm.astype(f32), pos_f])
        small = lax.all_gather(small, SHARD_AXES, axis=0)
        gain1 = small[:, 0].reshape(-1)
        gain2 = small[:, 1].reshape(-1)
        pos_own = positions.astype(f32)
        pos_oth = jnp.where(lax.axis_index("cp") == 0, small[1, 2, :seq], small[0, 2, :seq])

        full_qkv = gather_weight(jnp.concatenate(
            [w_q.reshape(rows, q_cols), w_k.reshape(rows, kv_cols), w_v.reshape(rows, kv_cols)], axis=1))
        full_o = gather_weight(w_o)
        full_gate = gather_weight(w_gate)
        full_up = gather_weight(w_up)
        full_down = gather_weight(w_down)

        half = head_dim // 2
        inv_freq = jnp.power(ROPE_THETA, -(jnp.arange(half, dtype=f32) * (2.0 / head_dim)))
        angle = pos_own[:, None] * inv_freq[None, :]
        cos_t, sin_t = jnp.cos(angle), jnp.sin(angle)
        cos_t = jnp.concatenate([cos_t] * 4, axis=1)
        sin_t = jnp.concatenate([-sin_t, sin_t, -sin_t, sin_t], axis=1)
        cos_4, sin_4 = jnp.concatenate([cos_t] * 4, axis=0), jnp.concatenate([sin_t] * 4, axis=0)
        pos_keys = jnp.concatenate([pos_own, pos_oth])
        mask = (pos_keys[None, :] <= pos_own[:, None]).astype(f32)
        mask_4 = jnp.concatenate([mask] * 4, axis=0)

        whole = lambda arr: pl.BlockSpec(arr.shape, lambda b: (0, 0))
        q_blk = pl.BlockSpec((seq, q_cols), lambda b: (b, 0))
        kv_blk = pl.BlockSpec((seq, 2 * kv_cols), lambda b: (b, 0))
        t_blk = 4 * seq
        kv_in_blk = pl.BlockSpec((t_blk, 2 * kv_cols), lambda b: (b, q_cols // (2 * kv_cols)))
        kv_tall = pl.BlockSpec((t_blk, 2 * kv_cols), lambda b: (b, 0))
        pair_flops = 2 * tokens * heads * head_dim * 2 * seq

        normed, rms1 = norm_fwd(x, gain1)
        qkv = matmul("td,dn->tn", normed, full_qkv)
        kv = pl.pallas_call(
            rope_kv_kernel, grid=(tokens // t_blk,),
            in_specs=[kv_in_blk, whole(cos_t), whole(sin_t)], out_specs=kv_tall,
            out_shape=jax.ShapeDtypeStruct((tokens, 2 * kv_cols), bf16),
            compiler_params=params(), cost_estimate=cost(1e9, 6e6), name="rope_kv",
        )(qkv, cos_t, sin_t)
        kv_oth = swap(kv, SWAP_Y)
        ctx, query = pl.pallas_call(
            functools.partial(attn_fwd_kernel, scale), grid=(batch,),
            in_specs=[q_blk, kv_blk, kv_blk, whole(cos_4), whole(sin_4), whole(mask_4)],
            out_specs=[q_blk, q_blk],
            out_shape=[jax.ShapeDtypeStruct((tokens, q_cols), bf16)] * 2,
            compiler_params=params(), cost_estimate=cost(4 * pair_flops, 40e6), name="attn_fwd",
        )(qkv, kv, kv_oth, cos_4, sin_4, mask_4)
        resid = (x.astype(f32) + matmul("tn,nd->td", ctx, full_o)).astype(bf16)
        normed2, rms2 = norm_fwd(resid, gain2)
        gate_pre = matmul("td,df->tf", normed2, full_gate)
        up_pre = matmul("td,df->tf", normed2, full_up)
        gate_sig = jax.nn.sigmoid(gate_pre)
        gate_act = gate_pre * gate_sig
        hidden = (gate_act * up_pre).astype(bf16)

        grad_down = matmul("tf,td->fd", hidden, dy) * share
        grad_down, dy, hidden = lax.optimization_barrier((grad_down, dy, hidden))
        grad_down = scatter_grad(grad_down)
        d_hidden = matmul("td,fd->tf", dy, full_down)
        d_gate = (d_hidden * up_pre * gate_sig * (1.0 + gate_pre * (1.0 - gate_sig))).astype(bf16)
        d_up = (d_hidden * gate_act).astype(bf16)
        blocks2 = relative_blocks(normed2, "y")
        gate_oth = partner_part(blocks2, d_gate, share)
        gate_oth, d_up = lax.optimization_barrier((gate_oth, d_up))
        gate_got = swap(gate_oth, SWAP_CORE)
        grad_up = matmul("td,tf->df", normed2, d_up) * share
        grad_up, d_gate, hidden = lax.optimization_barrier((grad_up, d_gate, hidden))
        grad_up = scatter_grad(grad_up)
        gate_far, gate_near = own_parts(blocks2, d_gate, gate_got, share)
        gate_far, gate_near, d_gate, d_up = lax.optimization_barrier((gate_far, gate_near, d_gate, d_up))
        gate_got = swap(gate_far, SWAP_Y)
        d_normed2 = matmul("tf,df->td", d_gate, full_gate)
        d_normed2 = d_normed2 + matmul("tf,df->td", d_up, full_up)
        d_resid, grad_ffn = norm_bwd(d_normed2, resid, rms2, gain2)
        d_resid = d_resid + dy.astype(f32)
        d_resid_half = d_resid.astype(bf16)
        blocks_o = relative_blocks(ctx, "y")
        o_oth = partner_part(blocks_o, d_resid_half, share)
        o_oth, d_resid_half = lax.optimization_barrier((o_oth, d_resid_half))
        o_got = swap(o_oth, SWAP_CORE)
        d_ctx = matmul("td,nd->tn", d_resid_half, full_o).astype(bf16)
        d_ctx, d_resid_half = lax.optimization_barrier((d_ctx, d_resid_half))
        o_far, o_near = own_parts(blocks_o, d_resid_half, o_got, share)
        o_far, o_near, d_ctx = lax.optimization_barrier((o_far, o_near, d_ctx))
        dq_wide, dkv_own, dkv_oth = pl.pallas_call(
            functools.partial(attn_bwd_kernel, scale), grid=(batch,),
            in_specs=[q_blk, q_blk, kv_blk, kv_blk, whole(cos_4), whole(sin_4), whole(mask_4)],
            out_specs=[q_blk, kv_blk, kv_blk],
            out_shape=[jax.ShapeDtypeStruct((tokens, q_cols + 2 * kv_cols), bf16)]
            + [jax.ShapeDtypeStruct((tokens, 2 * kv_cols), f32)] * 2,
            compiler_params=params(), cost_estimate=cost(10 * pair_flops, 50e6), name="attn_bwd",
        )(query, d_ctx, kv, kv_oth, cos_4, sin_4, mask_4)
        dkv_got = swap(dkv_oth, SWAP_Y)
        o_got = swap(o_far, SWAP_Y)
        cut = q_cols // 2
        dq_parts = (dq_wide[:, :cut], dq_wide[:, cut:q_cols])
        q_blocks = (relative_blocks(normed, "x"), relative_blocks(normed, "y"))
        q_oth = [partner_part(blocks, part, share) for blocks, part in zip(q_blocks, dq_parts)]
        q_oth[0], q_oth[1], hidden = lax.optimization_barrier((q_oth[0], q_oth[1], hidden))
        q_got = [swap(part, SWAP_CORE) for part in q_oth]
        act_out = (resid.astype(f32) + matmul("tf,fd->td", hidden, full_down)).astype(bf16)
        act_out, dq_parts = lax.optimization_barrier((act_out, dq_parts))
        q_both = [own_parts(*args, share) for args in zip(q_blocks, dq_parts, q_got)]
        q_both, gate_near = lax.optimization_barrier((q_both, gate_near))
        q_got = [swap(q_both[0][0], SWAP_X), swap(q_both[1][0], SWAP_Y)]
        cut = rows
        gate_send = gate_near[cut:] + gate_got[cut:]
        gate_last = swap(gate_send, SWAP_X)
        o_send = o_near[cut:] + o_got[cut:]
        o_last = swap(o_send, SWAP_X)
        d_qkv = pl.pallas_call(
            unrope_kv_kernel, grid=(tokens // t_blk,),
            in_specs=[kv_tall, kv_tall, whole(cos_t), whole(sin_t), pl.BlockSpec(memory_space=pl.ANY)],
            out_specs=kv_in_blk,
            out_shape=jax.ShapeDtypeStruct(dq_wide.shape, bf16),
            input_output_aliases={4: 0},
            compiler_params=params(), cost_estimate=cost(1e9, 10e6), name="unrope_kv",
        )(dkv_own, dkv_got, cos_t, sin_t, dq_wide)
        grad_kv = matmul("td,tn->dn", normed, d_qkv[:, q_cols:]) * share
        grad_kv, d_qkv = lax.optimization_barrier((grad_kv, d_qkv))
        grad_kv = scatter_grad(grad_kv)
        q_send = [both[1][cut:] + got[cut:] for both, got in zip(q_both, q_got)]
        q_last = [swap(q_send[0], SWAP_Y), swap(q_send[1], SWAP_X)]
        d_normed = matmul("tn,dn->td", d_qkv, full_qkv)
        d_input, grad_attn = norm_bwd(d_normed, x, rms1, gain1)
        grad_in = (d_resid + d_input).astype(bf16)
        gains = jnp.stack([grad_attn.reshape(n_dev, rows), grad_ffn.reshape(n_dev, rows)], axis=1)
        gains = lax.psum_scatter(gains, SHARD_AXES, scatter_dimension=0, tiled=True)[0] * share
        grad_gate = gate_near[:cut] + gate_got[:cut] + gate_last
        grad_o = o_near[:cut] + o_got[:cut] + o_last
        grad_q = jnp.concatenate([both[1][:cut] + got[:cut] + last
                                  for both, got, last in zip(q_both, q_got, q_last)], axis=1).reshape(w_q.shape)
        grad_k = grad_kv[:, :kv_cols].reshape(w_k.shape)
        grad_v = grad_kv[:, kv_cols:].reshape(w_v.shape)
        shape = act_in.shape
        return (act_out.reshape(shape), grad_in.reshape(shape), gains[0], grad_q, grad_k, grad_v, grad_o, gains[1],
                grad_gate, grad_up, grad_down)

    in_specs = (act_spec, act_spec, P("cp"), vec_spec, cube_spec, cube_spec, cube_spec, mat_spec, vec_spec, mat_spec, mat_spec, mat_spec)
    out_specs = (act_spec, act_spec, vec_spec, cube_spec, cube_spec, cube_spec, mat_spec, vec_spec, mat_spec, mat_spec, mat_spec)
    return jax.shard_map(body, mesh=mesh, in_specs=in_specs, out_specs=out_specs, check_vma=False)
```

```python
import functools

import jax
import jax.numpy as jnp
from jax import lax
from jax.experimental import pallas as pl
from jax.experimental.pallas import tpu as pltpu
from jax.sharding import PartitionSpec as P


NORM_EPS = 1e-5
ROPE_THETA = 500000.0
NEG_INF = -1e30
SHARD_AXES = ("fsdp", "cp")
LANES = 128
HALF_SLAB = 64


def matmul(form, lhs, rhs):
    return jnp.einsum(form, lhs, rhs, preferred_element_type=jnp.float32)


def dims(lhs_dim, rhs_dim):
    return (((lhs_dim,), (rhs_dim,)), ((), ()))


def kdot(lhs, rhs, lhs_dim, rhs_dim):
    return lax.dot_general(lhs, rhs, dims(lhs_dim, rhs_dim), preferred_element_type=jnp.float32)


def lane_of(rows):
    return lax.broadcasted_iota(jnp.int32, (rows, LANES), 1)


def partner_half(vals):
    low = (lane_of(vals.shape[0]) % 64) < 32
    return jnp.where(low, pltpu.roll(vals, LANES - 32, 1), pltpu.roll(vals, 32, 1))


def pair_blocks(slab, odd):
    wide = slab.astype(jnp.float32)
    low = lane_of(wide.shape[0]) < HALF_SLAB
    mine = jnp.where(low, 0.0, wide) if odd else jnp.where(low, wide, 0.0)
    moved = pltpu.roll(mine, HALF_SLAB, 1)
    parts = (moved, mine) if odd else (mine, moved)
    return jnp.concatenate(parts, axis=0).astype(jnp.bfloat16)


def rope_kv_kernel(kv_ref, cos_ref, sin_ref, out_ref):
    reps = kv_ref.shape[0] // cos_ref.shape[0]
    cos_t = jnp.concatenate([cos_ref[...]] * reps, axis=0)
    sin_t = jnp.concatenate([sin_ref[...]] * reps, axis=0)
    for j in range(2):
        cols = slice(j * LANES, (j + 1) * LANES)
        vals = kv_ref[:, cols]
        out_ref[:, cols] = (vals * cos_t + partner_half(vals) * sin_t).astype(jnp.bfloat16)
    out_ref[:, 2 * LANES:] = kv_ref[:, 2 * LANES:].astype(jnp.bfloat16)


def unrope_kv_kernel(own_ref, got_ref, cos_ref, sin_ref, wide_ref, out_ref):
    del wide_ref
    reps = own_ref.shape[0] // cos_ref.shape[0]
    cos_t = jnp.concatenate([cos_ref[...]] * reps, axis=0)
    sin_t = jnp.concatenate([sin_ref[...]] * reps, axis=0)
    for j in range(2):
        cols = slice(j * LANES, (j + 1) * LANES)
        vals = own_ref[:, cols] + got_ref[:, cols]
        out_ref[:, cols] = (vals * cos_t - partner_half(vals) * sin_t).astype(jnp.bfloat16)
    out_ref[:, 2 * LANES:] = (own_ref[:, 2 * LANES:] + got_ref[:, 2 * LANES:]).astype(jnp.bfloat16)


def stack_slabs(ref, group):
    return jnp.concatenate([ref[:, pl.ds((group * 4 + j) * LANES, LANES)] for j in range(4)], axis=0)


def write_slabs(ref, group, vals):
    rows = vals.shape[0] // 4
    for j in range(4):
        ref[:, pl.ds((group * 4 + j) * LANES, LANES)] = vals[j * rows:(j + 1) * rows].astype(ref.dtype)


def kv_pair(kv_ref, kvo_ref, group):
    at = (group // 2) * LANES
    odd = group % 2 == 1
    key = jnp.concatenate([kv_ref[:, at:at + LANES], kvo_ref[:, at:at + LANES]], axis=0)
    at += 2 * LANES
    val = jnp.concatenate([kv_ref[:, at:at + LANES], kvo_ref[:, at:at + LANES]], axis=0)
    return pair_blocks(key, odd), pair_blocks(val, odd)


def softmax_pair(query, key2, mask, scale):
    scores = kdot(query, key2, 1, 1) * scale
    probs = []
    for j in range(2):
        part = jnp.where(mask, scores[:, j * LANES:(j + 1) * LANES], NEG_INF)
        expo = jnp.exp(part - jnp.max(part, axis=1, keepdims=True))
        probs.append(expo * (1.0 / jnp.sum(expo, axis=1, keepdims=True)))
    return probs


def attn_fwd_kernel(scale, q_ref, kv_ref, kvo_ref, cos_ref, sin_ref, mask_ref, ctx_ref, qb_ref):
    mask = mask_ref[...] > 0.0
    for group in range(4):
        key2, val2 = kv_pair(kv_ref, kvo_ref, group)
        raw = stack_slabs(q_ref, group)
        query = (raw * cos_ref[...] + partner_half(raw) * sin_ref[...]).astype(jnp.bfloat16)
        write_slabs(qb_ref, group, query)
        probs = softmax_pair(query, key2, mask, scale)
        prob = jnp.concatenate([part.astype(jnp.bfloat16) for part in probs], axis=1)
        write_slabs(ctx_ref, group, kdot(prob, val2, 1, 0))


def attn_bwd_kernel(scale, qb_ref, dc_ref, kv_ref, kvo_ref, cos_ref, sin_ref, mask_ref, dq_ref, own_ref, oth_ref):
    mask = mask_ref[...] > 0.0
    keys = 2 * kv_ref.shape[0]
    local = kv_ref.shape[0]
    low = lane_of(keys) < HALF_SLAB
    held = {}
    for group in range(4):
        key2, val2 = kv_pair(kv_ref, kvo_ref, group)
        query = stack_slabs(qb_ref, group)
        d_ctx = stack_slabs(dc_ref, group)
        probs = softmax_pair(query, key2, mask, scale)
        d_prob = kdot(d_ctx, val2, 1, 1)
        d_scores = []
        for j in range(2):
            part = d_prob[:, j * LANES:(j + 1) * LANES]
            inner = jnp.sum(probs[j] * part, axis=1, keepdims=True)
            d_scores.append((probs[j] * (part - inner) * scale).astype(jnp.bfloat16))
        d_score = jnp.concatenate(d_scores, axis=1)
        prob = jnp.concatenate([part.astype(jnp.bfloat16) for part in probs], axis=1)
        d_query = kdot(d_score, key2, 1, 0)
        write_slabs(dq_ref, group, d_query * cos_ref[...] - partner_half(d_query) * sin_ref[...])
        for which, (lhs, rhs) in enumerate(((d_score, query), (prob, d_ctx))):
            both = kdot(lhs, rhs, 0, 0)
            top, bottom = both[:keys], both[keys:]
            if group % 2 == 0:
                held[which] = top + pltpu.roll(bottom, HALF_SLAB, 1)
            else:
                slab = jnp.where(low, held[which], bottom + pltpu.roll(top, HALF_SLAB, 1))
                at = (2 * which + group // 2) * LANES
                own_ref[:, at:at + LANES] = slab[:local]
                oth_ref[:, at:at + LANES] = slab[local:]


def cost(flops, nbytes):
    return pl.CostEstimate(flops=int(flops), bytes_accessed=int(nbytes), transcendentals=0)


VMEM_LIMIT = 48 * 1024 * 1024


def params():
    return pltpu.CompilerParams(dimension_semantics=("arbitrary",), vmem_limit_bytes=VMEM_LIMIT)


def norm_fwd(hidden, gain):
    hid32 = hidden.astype(jnp.float32)
    inv_rms = lax.rsqrt(jnp.mean(hid32 * hid32, axis=-1, keepdims=True) + NORM_EPS)
    return (hid32 * inv_rms * gain).astype(jnp.bfloat16), inv_rms


def norm_bwd(d_normed, hidden, inv_rms, gain):
    unit = hidden.astype(jnp.float32) * inv_rms
    d_unit = d_normed * gain
    d_hidden = inv_rms * (d_unit - unit * jnp.mean(d_unit * unit, axis=-1, keepdims=True))
    return d_hidden, jnp.sum(d_normed * unit, axis=0)


def gather_weight(shard):
    return lax.all_gather(shard, SHARD_AXES, axis=0, tiled=True)


def scatter_grad(local_grad):
    return lax.psum_scatter(local_grad, SHARD_AXES, scatter_dimension=0, tiled=True)


SWAP_CORE = ("fsdp", [(0, 1), (1, 0), (2, 3), (3, 2)])
SWAP_X = ("fsdp", [(0, 2), (2, 0), (1, 3), (3, 1)])
SWAP_Y = ("cp", [(0, 1), (1, 0)])


def swap(vals, how):
    return lax.ppermute(vals, how[0], how[1])


def place():
    at = lax.axis_index("fsdp")
    return at // 2, at % 2, lax.axis_index("cp")


def relative_blocks(lhs):
    block = lhs.shape[1] // 8
    x_at, core, y_at = place()
    sides = []
    for d_core in (0, 1):
        parts = []
        for d_y in (0, 1):
            for d_x in (0, 1):
                owner = (((x_at + d_x) % 2) * 2 + (core + d_core) % 2) * 2 + (y_at + d_y) % 2
                parts.append(lax.dynamic_slice_in_dim(lhs, owner * block + block // 2, block // 2, 1))
        sides.append(parts)
    return sides


def first_halves(lhs):
    block = lhs.shape[1] // 8
    return jnp.concatenate([lhs[:, i * block:i * block + block // 2] for i in range(8)], axis=1)


def core_blocks(lhs, d_core):
    block = lhs.shape[1] // 4
    x_at, core, _ = place()
    starts = [(((x_at + d_x) % 2) * 2 + (core + d_core) % 2) * block for d_x in (0, 1)]
    return jnp.concatenate([lax.dynamic_slice_in_dim(lhs, at, block, 1) for at in starts], axis=1)


def partner_part(blocks, rhs, scale):
    return matmul("td,tn->dn", jnp.concatenate(blocks[1], axis=1), rhs) * scale


def own_parts(blocks, rhs, got, scale):
    cut = got.shape[0] // 2
    far = matmul("td,tn->dn", jnp.concatenate(blocks[0][2:], axis=1), rhs) * scale + got[cut:]
    near = matmul("td,tn->dn", jnp.concatenate(blocks[0][:2], axis=1), rhs) * scale + got[:cut]
    return far, near


def solution(mesh):
    n_dev = mesh.shape["fsdp"] * mesh.shape["cp"]
    act_spec = P("fsdp", "cp", None)
    vec_spec = P(SHARD_AXES)
    mat_spec = P(SHARD_AXES, None)
    cube_spec = P(SHARD_AXES, None, None)
    bf16, f32 = jnp.bfloat16, jnp.float32

    def body(act_in, grad_out, positions, attn_norm, w_q, w_k, w_v, w_o, ffn_norm, w_gate, w_up, w_down):
        batch, seq, width = act_in.shape
        heads, head_dim = w_q.shape[1], w_q.shape[2]
        kv_heads = w_k.shape[1]
        rows = w_q.shape[0]
        q_cols, kv_cols = heads * head_dim, kv_heads * head_dim
        tokens = batch * seq
        scale = head_dim ** -0.5
        share = 1.0 / n_dev
        x = act_in.reshape(tokens, width)
        dy = grad_out.reshape(tokens, width)

        pos_f = jnp.concatenate([positions.astype(f32), jnp.zeros((rows - seq,), f32)])
        small = jnp.stack([attn_norm.astype(f32), ffn_norm.astype(f32), pos_f])
        small = lax.all_gather(small, SHARD_AXES, axis=0)
        gain1 = small[:, 0].reshape(-1)
        gain2 = small[:, 1].reshape(-1)
        pos_own = positions.astype(f32)
        pos_oth = jnp.where(lax.axis_index("cp") == 0, small[1, 2, :seq], small[0, 2, :seq])

        full_qkv = gather_weight(jnp.concatenate(
            [w_q.reshape(rows, q_cols), w_k.reshape(rows, kv_cols), w_v.reshape(rows, kv_cols)], axis=1))
        full_o = gather_weight(w_o)
        full_gate = gather_weight(w_gate)
        full_up = gather_weight(w_up)
        full_down = gather_weight(w_down)

        half = head_dim // 2
        inv_freq = jnp.power(ROPE_THETA, -(jnp.arange(half, dtype=f32) * (2.0 / head_dim)))
        angle = pos_own[:, None] * inv_freq[None, :]
        cos_t, sin_t = jnp.cos(angle), jnp.sin(angle)
        cos_t = jnp.concatenate([cos_t] * 4, axis=1)
        sin_t = jnp.concatenate([-sin_t, sin_t, -sin_t, sin_t], axis=1)
        cos_4, sin_4 = jnp.concatenate([cos_t] * 4, axis=0), jnp.concatenate([sin_t] * 4, axis=0)
        pos_keys = jnp.concatenate([pos_own, pos_oth])
        mask = (pos_keys[None, :] <= pos_own[:, None]).astype(f32)
        mask_4 = jnp.concatenate([mask] * 4, axis=0)

        whole = lambda arr: pl.BlockSpec(arr.shape, lambda b: (0, 0))
        q_blk = pl.BlockSpec((seq, q_cols), lambda b: (b, 0))
        kv_blk = pl.BlockSpec((seq, 2 * kv_cols), lambda b: (b, 0))
        t_blk = 4 * seq
        kv_in_blk = pl.BlockSpec((t_blk, 2 * kv_cols), lambda b: (b, q_cols // (2 * kv_cols)))
        kv_tall = pl.BlockSpec((t_blk, 2 * kv_cols), lambda b: (b, 0))
        pair_flops = 2 * tokens * heads * head_dim * 2 * seq

        normed, rms1 = norm_fwd(x, gain1)
        qkv = matmul("td,dn->tn", normed, full_qkv)
        kv = pl.pallas_call(
            rope_kv_kernel, grid=(tokens // t_blk,),
            in_specs=[kv_in_blk, whole(cos_t), whole(sin_t)], out_specs=kv_tall,
            out_shape=jax.ShapeDtypeStruct((tokens, 2 * kv_cols), bf16),
            compiler_params=params(), cost_estimate=cost(1e9, 6e6), name="rope_kv",
        )(qkv, cos_t, sin_t)
        kv_oth = swap(kv, SWAP_Y)
        ctx, query = pl.pallas_call(
            functools.partial(attn_fwd_kernel, scale), grid=(batch,),
            in_specs=[q_blk, kv_blk, kv_blk, whole(cos_4), whole(sin_4), whole(mask_4)],
            out_specs=[q_blk, q_blk],
            out_shape=[jax.ShapeDtypeStruct((tokens, q_cols), bf16)] * 2,
            compiler_params=params(), cost_estimate=cost(4 * pair_flops, 40e6), name="attn_fwd",
        )(qkv, kv, kv_oth, cos_4, sin_4, mask_4)
        resid = (x.astype(f32) + matmul("tn,nd->td", ctx, full_o)).astype(bf16)
        normed2, rms2 = norm_fwd(resid, gain2)
        normed2, blocks2, lhs_a = lax.optimization_barrier((normed2, relative_blocks(normed2), first_halves(normed2)))
        gate_pre = matmul("td,df->tf", normed2, full_gate)
        up_pre = matmul("td,df->tf", normed2, full_up)
        gate_sig = jax.nn.sigmoid(gate_pre)
        gate_act = gate_pre * gate_sig
        hidden = (gate_act * up_pre).astype(bf16)

        half_w = width // 2
        down_oth = matmul("tf,td->fd", core_blocks(hidden, 1), dy[:, half_w:]) * share
        down_oth, hidden, dy = lax.optimization_barrier((down_oth, hidden, dy))
        down_got = swap(down_oth, SWAP_CORE)
        down_a = matmul("tf,td->fd", hidden, dy[:, :half_w]) * share
        down_a, hidden, dy = lax.optimization_barrier((down_a, hidden, dy))
        down_a = scatter_grad(down_a)
        down_own = matmul("tf,td->fd", core_blocks(hidden, 0), dy[:, half_w:]) * share + down_got
        down_own, hidden, dy = lax.optimization_barrier((down_own, hidden, dy))
        y_at = place()[2]
        down_own = down_own.reshape(2, 2, down_own.shape[0] // 4, half_w)
        down_far = lax.dynamic_slice_in_dim(down_own, 1 - y_at, 1, 1)
        down_far, dy = lax.optimization_barrier((down_far, dy))
        down_got = swap(down_far, SWAP_Y)
        d_hidden = matmul("td,fd->tf", dy, full_down)
        d_gate = (d_hidden * up_pre * gate_sig * (1.0 + gate_pre * (1.0 - gate_sig))).astype(bf16)
        d_up = (d_hidden * gate_act).astype(bf16)

        def split_grad(d_pre, after):
            oth = partner_part(blocks2, d_pre, share)
            oth, d_pre = lax.optimization_barrier((oth, d_pre))
            got = swap(oth, SWAP_CORE)
            whole_a = matmul("td,tn->dn", lhs_a, d_pre) * share
            whole_a, d_pre = lax.optimization_barrier((whole_a, d_pre))
            whole_a = scatter_grad(whole_a)
            far, near = own_parts(blocks2, d_pre, got, share)
            far, near, d_pre, after = lax.optimization_barrier((far, near, d_pre, after))
            got = swap(far, SWAP_Y)
            return whole_a, near, got, d_pre, after

        gate_a, gate_near, gate_got, d_gate, d_up = split_grad(d_gate, d_up)
        up_a, up_near, up_got, d_up, (d_gate, down_own) = split_grad(d_up, (d_gate, down_own))
        down_near = lax.dynamic_slice_in_dim(down_own, y_at, 1, 1)
        down_send = down_near[1] + down_got[1]
        down_last = swap(down_send, SWAP_X)
        d_normed2 = matmul("tf,df->td", d_gate, full_gate)
        d_normed2 = d_normed2 + matmul("tf,df->td", d_up, full_up)
        d_resid, grad_ffn = norm_bwd(d_normed2, resid, rms2, gain2)
        d_resid = d_resid + dy.astype(f32)
        d_resid_half = d_resid.astype(bf16)
        grad_o = matmul("tn,td->nd", ctx, d_resid_half) * share
        grad_o, d_resid_half = lax.optimization_barrier((grad_o, d_resid_half))
        grad_o = scatter_grad(grad_o)
        d_ctx = matmul("td,nd->tn", d_resid_half, full_o).astype(bf16)
        d_ctx, gate_near = lax.optimization_barrier((d_ctx, gate_near))
        cut = rows // 2
        gate_send = gate_near[cut:] + gate_got[cut:]
        gate_last = swap(gate_send, SWAP_X)
        dq_wide, dkv_own, dkv_oth = pl.pallas_call(
            functools.partial(attn_bwd_kernel, scale), grid=(batch,),
            in_specs=[q_blk, q_blk, kv_blk, kv_blk, whole(cos_4), whole(sin_4), whole(mask_4)],
            out_specs=[q_blk, kv_blk, kv_blk],
            out_shape=[jax.ShapeDtypeStruct((tokens, q_cols + 2 * kv_cols), bf16)]
            + [jax.ShapeDtypeStruct((tokens, 2 * kv_cols), f32)] * 2,
            compiler_params=params(), cost_estimate=cost(10 * pair_flops, 50e6), name="attn_bwd",
        )(query, d_ctx, kv, kv_oth, cos_4, sin_4, mask_4)
        dkv_got = swap(dkv_oth, SWAP_Y)
        grad_q = matmul("td,tn->dn", normed, dq_wide[:, :q_cols]) * share
        grad_q, hidden = lax.optimization_barrier((grad_q, hidden))
        grad_q = scatter_grad(grad_q)
        act_out = (resid.astype(f32) + matmul("tf,fd->td", hidden, full_down)).astype(bf16)
        act_out, up_near = lax.optimization_barrier((act_out, up_near))
        up_send = up_near[cut:] + up_got[cut:]
        up_send, dkv_own = lax.optimization_barrier((up_send, dkv_own))
        up_last = swap(up_send, SWAP_X)
        d_qkv = pl.pallas_call(
            unrope_kv_kernel, grid=(tokens // t_blk,),
            in_specs=[kv_tall, kv_tall, whole(cos_t), whole(sin_t), pl.BlockSpec(memory_space=pl.ANY)],
            out_specs=kv_in_blk,
            out_shape=jax.ShapeDtypeStruct(dq_wide.shape, bf16),
            input_output_aliases={4: 0},
            compiler_params=params(), cost_estimate=cost(1e9, 10e6), name="unrope_kv",
        )(dkv_own, dkv_got, cos_t, sin_t, dq_wide)
        grad_kv = matmul("td,tn->dn", normed, d_qkv[:, q_cols:]) * share
        grad_kv, d_qkv = lax.optimization_barrier((grad_kv, d_qkv))
        grad_kv = scatter_grad(grad_kv)
        d_normed = matmul("tn,dn->td", d_qkv, full_qkv)
        d_input, grad_attn = norm_bwd(d_normed, x, rms1, gain1)
        grad_in = (d_resid + d_input).astype(bf16)
        gains = jnp.stack([grad_attn.reshape(n_dev, rows), grad_ffn.reshape(n_dev, rows)], axis=1)
        gains = lax.psum_scatter(gains, SHARD_AXES, scatter_dimension=0, tiled=True)[0] * share
        grad_down = jnp.concatenate([down_a, (down_near[0] + down_got[0] + down_last)[0]], axis=1)
        grad_gate = jnp.concatenate([gate_a, gate_near[:cut] + gate_got[:cut] + gate_last], axis=0)
        grad_up = jnp.concatenate([up_a, up_near[:cut] + up_got[:cut] + up_last], axis=0)
        grad_q = grad_q.reshape(w_q.shape)
        grad_k = grad_kv[:, :kv_cols].reshape(w_k.shape)
        grad_v = grad_kv[:, kv_cols:].reshape(w_v.shape)
        shape = act_in.shape
        return (act_out.reshape(shape), grad_in.reshape(shape), gains[0], grad_q, grad_k, grad_v, grad_o, gains[1],
                grad_gate, grad_up, grad_down)

    in_specs = (act_spec, act_spec, P("cp"), vec_spec, cube_spec, cube_spec, cube_spec, mat_spec, vec_spec, mat_spec, mat_spec, mat_spec)
    out_specs = (act_spec, act_spec, vec_spec, cube_spec, cube_spec, cube_spec, mat_spec, vec_spec, mat_spec, mat_spec, mat_spec)
    return jax.shard_map(body, mesh=mesh, in_specs=in_specs, out_specs=out_specs, check_vma=False)
```
